512 devices in a mesh: dom: 32 (over y, x), feat: 16 (over z, core).
Axes of the slice: x: 4, y: 8, z: 8, core: 2. Of those that a mesh axis runs over, the one named last changes fastest.
Arguments:
- features: bfloat16 [128, 524288], P('feat', 'dom'), may hold values from -6 to 6
- seed_rows: int32 [8192], P('dom'), may hold values from 0 to 16383
- want_rows: int32 [32, 32, 128], P('dom'), may hold values from 0 to 16383
- live_counts: int32 [32, 32], P('dom'), may hold values from 1 to 128, as said below
- hop_one: int32 [15, 8192], P(None, 'dom'), may hold values from 0 to 4095, as said below
- hop_two: int32 [10, 15, 8192], P(None, None, 'dom'), may hold values from 0 to 4095, as said below
- w1_self: bfloat16 [256, 128], replicated, may hold values from -0.5 to 0.5
- w1_neigh: bfloat16 [256, 128], replicated, may hold values from -0.5 to 0.5
- b1: float32 [256], P('feat'), may hold values from -4 to 4
- w2_self: bfloat16 [256, 256], P(None, 'feat'), may hold values from -0.375 to 0.375
- w2_neigh: bfloat16 [256, 256], P(None, 'feat'), may hold values from -0.375 to 0.375
- b2: float32 [256], P('feat'), may hold values from -4 to 4
Outputs:
- embed: float32 [256, 8192], P('feat', 'dom')
The draws below stay inside these ranges and needn't reach their ends.
Inputs may be any that keep to these rules, and one draw needn't show every extreme that they name: `want_rows`: slots at or beyond live_counts[r, o] are ignored. `live_counts`: in every draw a quarter of the owners, every fourth one from a drawn offset, receive all 128 slots from every requester. `hop_one`: each entry is o * 128 + c, a position in the buffer of the requester that holds seed s, with c < live_counts of that requester and owner o. `hop_two`: each entry is o * 128 + c, a position in the buffer of the requester that holds seed s, with c < live_counts of that requester and owner o.
All inputs are finite; a program needn't handle non-finite values.
Results may differ from the reference program's by a relative error of at most 0.00036.
Values may be sent and summed in bfloat16 or wider, within the bound.
A program may use at most 64 MiB of HBM per device.

```python
import jax
import jax.numpy as jnp
from jax import lax

FEAT = 128
HID = 256
OUT = 256
FAN1 = 15
FAN2 = 10
CAP = 128
SEED_DEV = 256
NODE_DEV = 16384
OWNERS = 32
SEEDS = 8192
NODES = 524288


def slot_plan(key):
    offset = jax.random.randint(jax.random.fold_in(key, 501), (), 0, 4)
    owner = jnp.arange(OWNERS, dtype=jnp.int32)
    spread = jax.random.randint(jax.random.fold_in(key, 502), (OWNERS, OWNERS), CAP // 8, CAP + 1)
    full = ((owner - offset) % 4 == 0)[None, :]
    return (offset, jnp.where(full, CAP, spread).astype(jnp.int32))


def positions(key, salt, lead):
    offset, counts = slot_plan(key)
    draw_key = jax.random.fold_in(key, salt)
    shape = lead + (SEEDS,)
    requester = jnp.broadcast_to(jnp.arange(SEEDS, dtype=jnp.int32) // SEED_DEV, shape)
    choose = jax.random.randint(jax.random.fold_in(draw_key, 1), shape, 0, 2)
    favored = (offset + 4 * jax.random.randint(jax.random.fold_in(draw_key, 2), shape, 0, OWNERS // 4)) % OWNERS
    anyone = jax.random.randint(jax.random.fold_in(draw_key, 3), shape, 0, OWNERS)
    owner = jnp.where(choose == 1, favored, anyone).astype(jnp.int32)
    limit = counts[requester, owner]
    slot = jax.random.randint(jax.random.fold_in(draw_key, 4), shape, 0, 1 << 20) % limit
    return (owner * CAP + slot).astype(jnp.int32)


def draw_live_counts(key, part):
    return slot_plan(key)[1]


def draw_hop_one(key, part):
    return positions(key, 11, (FAN1,))


def draw_hop_two(key, part):
    return positions(key, 12, (FAN2, FAN1))


def plant(values, stream_key, least, top_value):
    spot = [jax.random.randint(jax.random.fold_in(stream_key, axis), (), 0, length) for axis, length in enumerate(values.shape)]
    widest = values.shape.index(max(values.shape))
    neighbour = spot[:widest] + [(spot[widest] + 1) % values.shape[widest]] + spot[widest + 1:]
    return values.at[tuple(spot)].set(least).at[tuple(neighbour)].set(top_value)


def block_levels(rng, dims, cuts, least, top_value):
    gain = 1.0
    for axis_at, blocks in cuts:
        steps = jax.random.uniform(jax.random.fold_in(jax.random.fold_in(rng, 6), axis_at), (blocks,), jnp.float32, least / len(cuts), top_value / len(cuts))
        gain = gain * jnp.repeat(jnp.exp(steps), dims[axis_at] // blocks).reshape((-1,) + (1,) * (len(dims) - 1 - axis_at))
    return gain


def centred(own_key, dims, scale, most, pieces=(), kind=jnp.bfloat16):
    level = block_levels(own_key, dims, pieces, -0.22, 0.18) if pieces else 1.0
    entries = jax.random.normal(own_key, dims, jnp.float32) * scale * level
    return jnp.minimum(jnp.maximum(entries, -most), most).astype(kind)


def setup_inputs(seed: int = 0) -> dict:
    arg_keys = jax.random.split(jax.random.key(seed), 13)
    features = centred(arg_keys[0], (FEAT, NODES), 1.0, 6.0, ((0, 16), (1, 32)))
    seed_rows = plant(jax.random.randint(arg_keys[1], (SEEDS,), 0, NODE_DEV), jax.random.fold_in(arg_keys[1], 1), 0, NODE_DEV - 1).astype(jnp.int32)
    want_rows = plant(jax.random.randint(arg_keys[2], (OWNERS, OWNERS, CAP), 0, NODE_DEV), jax.random.fold_in(arg_keys[2], 1), 0, NODE_DEV - 1).astype(jnp.int32)
    live_counts = draw_live_counts(jax.random.fold_in(arg_keys[12], 71), 0)
    hop_one = draw_hop_one(jax.random.fold_in(arg_keys[12], 71), 0)
    hop_two = draw_hop_two(jax.random.fold_in(arg_keys[12], 71), 0)
    w1_self = centred(arg_keys[6], (HID, FEAT), FEAT ** -0.5, 0.5)
    w1_neigh = centred(arg_keys[7], (HID, FEAT), FEAT ** -0.5, 0.5)
    b1 = centred(arg_keys[8], (HID,), 1.0, 4.0, ((0, 16),), jnp.float32)
    w2_self = centred(arg_keys[9], (OUT, HID), HID ** -0.5, 0.375, ((1, 16),))
    w2_neigh = centred(arg_keys[10], (OUT, HID), HID ** -0.5, 0.375, ((1, 16),))
    b2 = centred(arg_keys[11], (OUT,), 1.0, 4.0, ((0, 16),), jnp.float32)
    return {"features": features, "seed_rows": seed_rows, "want_rows": want_rows, "live_counts": live_counts, "hop_one": hop_one, "hop_two": hop_two, "w1_self": w1_self, "w1_neigh": w1_neigh, "b1": b1, "w2_self": w2_self, "w2_neigh": w2_neigh, "b2": b2}


def reference(features, seed_rows, want_rows, live_counts, hop_one, hop_two, w1_self, w1_neigh, b1, w2_self, w2_neigh, b2):
    owner = jnp.arange(OWNERS, dtype=jnp.int32)
    nodes = want_rows + (owner * NODE_DEV)[None, :, None]
    fetched = jnp.take(features, nodes.reshape(-1).astype(jnp.int32), axis=1)
    slot = jnp.arange(CAP, dtype=jnp.int32)
    live = slot[None, None, :] < live_counts[:, :, None]
    fetched = jnp.where(live.reshape(1, -1), fetched, jnp.zeros((), fetched.dtype))
    requester = jnp.arange(SEEDS, dtype=jnp.int32) // SEED_DEV
    base = requester * (OWNERS * CAP)
    x_one = jnp.take(fetched, (hop_one + base[None, :]).reshape(-1).astype(jnp.int32), axis=1)

    def add_hop(number, total):
        picked = jnp.take(fetched, (hop_two[number] + base[None, :]).reshape(-1).astype(jnp.int32), axis=1)
        return total + picked.astype(jnp.float32)
    m_two = lax.fori_loop(0, FAN2, add_hop, jnp.zeros((FEAT, FAN1 * SEEDS), jnp.float32))
    m_two = (m_two * (1.0 / FAN2)).astype(jnp.bfloat16)
    x_seed = jnp.take(features, (seed_rows + requester * NODE_DEV).astype(jnp.int32), axis=1)
    m_one = (lax.optimization_barrier(jnp.sum(x_one.reshape(FEAT, FAN1, SEEDS).astype(jnp.float32), axis=1)) * (1.0 / FAN1)).astype(jnp.bfloat16)

    def layer(selves, means):
        pre = jnp.dot(w1_self, selves, preferred_element_type=jnp.float32)
        pre = pre + jnp.dot(w1_neigh, means, preferred_element_type=jnp.float32) + b1[:, None]
        return jnp.maximum(pre, 0.0)
    h_one = layer(x_one, m_two)
    h_seed = layer(x_seed, m_one)
    g_mean = lax.optimization_barrier(jnp.sum(h_one.reshape(HID, FAN1, SEEDS), axis=1)) * (1.0 / FAN1)
    z_out = jnp.dot(w2_self.astype(jnp.float32), h_seed, precision=lax.Precision.HIGHEST, preferred_element_type=jnp.float32)
    z_out = z_out + jnp.dot(w2_neigh.astype(jnp.float32), g_mean, precision=lax.Precision.HIGHEST, preferred_element_type=jnp.float32) + b2[:, None]
    square = lax.optimization_barrier(jnp.sum(z_out * z_out, axis=0))
    return z_out * lax.rsqrt(square * (1.0 / OUT) + 1.0)
```

```python
import jax
import jax.numpy as jnp
from jax import lax
from jax.experimental import pallas as pl
from jax.experimental.pallas import tpu as pltpu
from jax.sharding import PartitionSpec as P

OUT = 256
FAN1 = 15
FAN2 = 10
CAP = 128
DOM = 32
FEAT_DEV = 16
RING = 8
CHUNKS = 4
PER = DOM // CHUNKS
MESH = pl.DeviceIdType.MESH
BF = jnp.bfloat16
F32 = jnp.float32


def iota(shape, dim):
    return lax.broadcasted_iota(jnp.int32, shape, dim)


def dot(a, b):
    return jnp.dot(a, b, preferred_element_type=F32)


def halves(x):
    high = x.astype(BF)
    return high, (x - high.astype(F32)).astype(BF)


def thirds(x):
    high = x.astype(BF)
    rest = x - high.astype(F32)
    mid = rest.astype(BF)
    return high, mid, (rest - mid.astype(F32)).astype(BF)


def swap_groups(x):
    row, group = iota((8, 128), 0), iota((8, 128), 1) // 16
    for bit in (1, 2, 4):
        down = pltpu.roll(pltpu.roll(x, bit, 0), 128 - 16 * bit, 1)
        up = pltpu.roll(pltpu.roll(x, 8 - bit, 0), 16 * bit, 1)
        low_row, low_group = (row & bit) == 0, (group & bit) == 0
        x = jnp.where(low_row == low_group, x, jnp.where(low_row, up, down))
    return x


def kernel(
    tab_ref, seed_ref, want_ref, live_ref, hop1_ref, hop2_ref, w1s_ref, w1n_ref, b1_ref, w2s_ref, w2n_ref, b2_ref,
    out_ref,
    table, wants, asked, picked, fetched, seeds_own, seeds_all, w2s_all, w2n_all, bias_own, bias_all, counts,
    outgoing, incoming,
    ask_send, ask_recv, pick_send, pick_recv, small_send, small_recv, ring_send, ring_recv, pair_send, pair_recv,
    last_send, last_recv,
):
    me_dom, me = lax.axis_index("dom"), lax.axis_index("feat")
    z, core = me // 2, lax.rem(me, 2)

    def remote(src, dst, send, recv, **where):
        return pltpu.make_async_remote_copy(
            src_ref=src, dst_ref=dst, send_sem=send, recv_sem=recv, device_id=where, device_id_type=MESH
        )

    barrier = pltpu.get_barrier_semaphore()

    def greet(i, _):
        pl.semaphore_signal(barrier, inc=1, device_id={"dom": lax.rem(me_dom + i, DOM)}, device_id_type=MESH)
        return 0

    def greet_feat(i, _):
        pl.semaphore_signal(barrier, inc=1, device_id={"feat": lax.rem(me + i, FEAT_DEV)}, device_id_type=MESH)
        return 0

    lax.fori_loop(1, DOM, greet, 0)
    lax.fori_loop(1, FEAT_DEV, greet_feat, 0)

    eye = iota((DOM, DOM), 0) == iota((DOM, DOM), 1)
    live = jnp.where(eye, jnp.broadcast_to(live_ref[...].astype(F32), (DOM, DOM)), 0.0)
    live = jnp.sum(live, axis=1, keepdims=True).astype(jnp.int32)
    asks = jnp.where(iota((DOM, CAP), 1) < live, want_ref[...], -1)
    wants[...] = asks.reshape(DOM, 1, CAP)

    spot = (iota((16, OUT), 1) == iota((16, OUT), 0) + 16 * me).astype(BF)
    for row, ref in enumerate((b1_ref, b2_ref)):
        placed = sum(dot(part, spot) for part in thirds(jnp.broadcast_to(ref[...], (8, 16))))
        bias_own[row : row + 1, :] = placed[0:1]

    for pair in range(32):
        left = tab_ref[:, pl.ds(512 * pair, 256)]
        right = tab_ref[:, pl.ds(512 * pair + 256, 256)]
        table[pl.ds(16 * pair, 16), :] = jnp.concatenate([left, right], axis=0)

    def pick(rows):
        low = jnp.where(rows >= 0, rows & 255, -1)
        high = jnp.broadcast_to(rows >> 8, (8, 256))
        chosen = (iota((256, 256), 0) == low).astype(BF)
        found = dot(table[...], chosen)
        parts = [found[8 * h : 8 * h + 8] for h in range(64)]
        for bit in range(6):
            upper = (high & (1 << bit)) != 0
            parts = [jnp.where(upper, parts[2 * i + 1], parts[2 * i]) for i in range(len(parts) // 2)]
        return parts[0].astype(BF)

    seeds_own[...] = pick(seed_ref[...])

    pl.semaphore_wait(barrier, DOM - 1 + FEAT_DEV - 1)

    def ask(i, _):
        to = lax.rem(me_dom + i, DOM)
        remote(wants.at[to], asked.at[me_dom], ask_send, ask_recv, dom=to).start()
        return 0

    own_ask = pltpu.make_async_copy(wants.at[me_dom], asked.at[me_dom], ask_recv)
    own_ask.start()
    lax.fori_loop(1, DOM, ask, 0)

    w2_rows = pl.ds(pl.multiple_of(16 * me, 16), 16)
    small = (
        (seeds_own, seeds_all.at[me]),
        (w2s_ref, w2s_all.at[w2_rows, :]),
        (w2n_ref, w2n_all.at[w2_rows, :]),
        (bias_own, bias_all.at[me]),
    )
    for kind, (src, dst) in enumerate(small):
        pltpu.make_async_copy(src, dst, small_recv.at[kind]).start()

    def spread(i, _):
        to = lax.rem(me + i, FEAT_DEV)
        for kind, (src, dst) in enumerate(small):
            remote(src, dst, small_send.at[kind], small_recv.at[kind], feat=to).start()
        return 0

    lax.fori_loop(1, FEAT_DEV, spread, 0)

    mine = (iota((256, 256), 0) == lax.rem(iota((256, 256), 1), 16) + 16 * me).astype(BF)
    keep = iota((FAN1, 256), 1) // 16 == iota((FAN1, 256), 0)

    def row_of(hops):
        high = dot((hops >> 7).astype(F32).astype(BF), mine)
        low = dot((hops & 127).astype(F32).astype(BF), mine)
        place = jnp.sum(jnp.where(keep, high * 128.0 + low, 0.0), axis=0, keepdims=True)
        place = jnp.where(iota((1, 256), 1) < 16 * FAN1, place, -1.0)
        return place.astype(jnp.int32)

    first = row_of(hop1_ref[...])
    second = [row_of(hop2_ref[k]) for k in range(FAN2)]
    first = jnp.broadcast_to(first, (8, 256))
    second = [jnp.broadcast_to(row, (8, 256)) for row in second]

    def count(block, _):
        ones, tens = [], []
        for half in range(2):
            place = iota((8, 256), 0) + (block * 16 + half * 8)
            ones.append((first == place).astype(F32))
            total = (second[0] == place).astype(F32)
            for row in second[1:]:
                total = total + (row == place).astype(F32)
            tens.append(total)
        rows = pl.ds(pl.multiple_of(block * 16, 16), 16)
        counts[rows, 0:256] = jnp.concatenate(ones, axis=0).astype(BF)
        counts[rows, 256:512] = jnp.concatenate(tens, axis=0).astype(BF)
        return 0

    lax.fori_loop(0, DOM * CAP // 16, count, 0)

    pltpu.make_async_copy(wants, asked, ask_recv).wait()

    def chunk_of(owner):
        return owner // PER

    def serve(i, _):
        base = 2 * lax.rem(me_dom // 2 + i, DOM // 2)
        rows = jnp.concatenate([asked[base], asked[base + 1]], axis=1)
        got = pick(rows)
        for half in range(2):
            to = base + half
            picked[to] = got[:, 128 * half : 128 * half + 128]
            mine_too = to == me_dom

            @pl.when(mine_too)
            def _():
                pltpu.make_async_copy(
                    picked.at[to], fetched.at[me_dom, me], pick_recv.at[chunk_of(me_dom)]
                ).start()

            @pl.when(jnp.logical_not(mine_too))
            def _():
                remote(
                    picked.at[to], fetched.at[me_dom, me], pick_send, pick_recv.at[chunk_of(me_dom)], dom=to
                ).start()

        return 0

    lax.fori_loop(0, DOM // 2, serve, 0)

    def owners(q):
        return pl.ds(PER * q, PER)

    def block(q, origin):
        return fetched.at[owners(q), origin]

    up, down = lax.rem(z + 1, RING) * 2 + core, lax.rem(z + RING - 1, RING) * 2 + core
    partner = 2 * z + 1 - core

    def reach(q, way):
        return 4 if (q + way) % 2 == 0 else 3

    def origin_of(way, hop):
        return lax.rem(z + (RING - hop if way == 0 else hop), RING) * 2 + core

    def pass_on(q, way, hop):
        return remote(
            block(q, origin_of(way, hop)),
            block(q, origin_of(way, hop)),
            ring_send.at[way, hop, q],
            ring_recv.at[way, hop, q],
            feat=up if way == 0 else down,
        )

    def to_partner(q, way, hop):
        slot = hop if way == 0 else 4 + hop
        at = block(q, origin_of(way, hop))
        return remote(at, at, pair_send.at[slot, q], pair_recv.at[slot, q], feat=partner)

    started = []

    def go(copy):
        copy.start()
        started.append(copy)

    for q in range(CHUNKS):
        pltpu.make_async_copy(block(q, 0), block(q, 1), pick_recv.at[q]).wait()
        for way in range(2):
            go(pass_on(q, way, 0))
        go(to_partner(q, 0, 0))
    for hop in range(1, 5):
        for q in range(CHUNKS):
            for way in range(2):
                if hop <= reach(q, way):
                    pass_on(q, way, hop - 1).wait_recv()
                    if hop < reach(q, way):
                        go(pass_on(q, way, hop))
                    go(to_partner(q, way, hop))

    total = jnp.zeros((128, 512), F32)
    for q in range(CHUNKS):
        to_partner(q, 0, 0).wait_recv()
        for hop in range(1, 5):
            for way in range(2):
                if hop <= reach(q, way):
                    to_partner(q, way, hop).wait_recv()
        for pair in range(PER // 2):
            o = PER * q + 2 * pair
            left = fetched[o].reshape(128, CAP)
            right = fetched[o + 1].reshape(128, CAP)
            total = total + dot(jnp.concatenate([left, right], axis=1), counts[pl.ds(o * CAP, 256), :])

    for kind, (whole, part) in enumerate(
        ((seeds_all, seeds_all), (w2s_all, w2s_all), (w2n_all, w2n_all), (bias_all, bias_all))
    ):
        pltpu.make_async_copy(whole, part, small_recv.at[kind]).wait()

    seed_lane = iota((256, 256), 1) - 16 * FAN1
    own_seeds = ((iota((256, 256), 0) == seed_lane + 16 * me) & (seed_lane >= 0)).astype(BF)
    selves = (total[:, :256] + dot(seeds_all[...].reshape(128, 256), own_seeds)).T
    sums = total[:, 256:].T
    one_sum = selves[0:16]
    for j in range(1, FAN1):
        one_sum = one_sum + selves[16 * j : 16 * j + 16]
    means = jnp.concatenate([sums[: 16 * FAN1] * (1.0 / FAN2), one_sum * (1.0 / FAN1)], axis=0).astype(BF)
    selves = selves.astype(BF)

    def nt(a, b):
        return lax.dot_general(a, b, (((1,), (1,)), ((), ())), preferred_element_type=F32)

    biases = jnp.sum(bias_all[...], axis=0)
    hidden = nt(selves, w1s_ref[...]) + nt(means, w1n_ref[...])
    hidden = jnp.maximum(hidden + biases[0:1], 0.0)
    g = hidden[0:16]
    for j in range(1, FAN1):
        g = g + hidden[16 * j : 16 * j + 16]
    g = g * (1.0 / FAN1)
    h_seed = hidden[16 * FAN1 :]
    z_out = biases[1:2]
    for part in halves(h_seed):
        z_out = z_out + dot(part, w2s_all[...])
    for part in halves(g):
        z_out = z_out + dot(part, w2n_all[...])
    square = jnp.sum(z_out * z_out, axis=1, keepdims=True)
    embed = z_out * lax.rsqrt(square * (1.0 / OUT) + 1.0)

    for a in range(2):
        for h in range(2):
            turned = swap_groups(embed[8 * a : 8 * a + 8, 128 * h : 128 * h + 128])
            outgoing[8 * h : 8 * h + 8, a, :] = turned

    pltpu.make_async_copy(outgoing.at[me], incoming.at[me], last_recv).start()

    def hand(i, _):
        to = lax.rem(me + i, FEAT_DEV)
        remote(outgoing.at[to], incoming.at[me], last_send, last_recv, feat=to).start()
        return 0

    lax.fori_loop(1, FEAT_DEV, hand, 0)
    pltpu.make_async_copy(outgoing, incoming, last_recv).wait()

    came = incoming[...].reshape(32, 128).T
    widen = (iota((32, 256), 1) // 8 == iota((32, 256), 0)).astype(BF)
    wide = sum(dot(part, widen) for part in thirds(came))
    lane = lax.rem(iota((16, 256), 1), 8)
    result = jnp.zeros((16, 256), F32)
    for b in range(8):
        result = result + jnp.where(lane == b, wide[16 * b : 16 * b + 16], 0.0)
    out_ref[...] = result

    for copy in started:
        copy.wait_send()
    others = pl.ds(0, DOM - 1)
    pltpu.make_async_copy(wants.at[others], wants.at[others], ask_send).wait()
    pltpu.make_async_copy(picked.at[others], picked.at[others], pick_send).wait()
    peers = pl.ds(0, FEAT_DEV - 1)
    rows = pl.ds(0, 16 * (FEAT_DEV - 1))
    pltpu.make_async_copy(seeds_all.at[peers], seeds_all.at[peers], small_send.at[0]).wait()
    pltpu.make_async_copy(w2s_all.at[rows, :], w2s_all.at[rows, :], small_send.at[1]).wait()
    pltpu.make_async_copy(w2n_all.at[rows, :], w2n_all.at[rows, :], small_send.at[2]).wait()
    pltpu.make_async_copy(bias_all.at[peers], bias_all.at[peers], small_send.at[3]).wait()
    pltpu.make_async_copy(outgoing.at[peers], outgoing.at[peers], last_send).wait()


def per_device(
    features, seed_rows, want_rows, live_counts, hop_one, hop_two, w1_self, w1_neigh, b1, w2_self, w2_neigh, b2
):
    vmem = pl.BlockSpec(memory_space=pltpu.VMEM)
    dma = pltpu.SemaphoreType.DMA
    return pl.pallas_call(
        kernel,
        out_shape=jax.ShapeDtypeStruct((16, 256), F32),
        in_specs=[vmem] * 12,
        out_specs=vmem,
        scratch_shapes=[
            pltpu.VMEM((512, 256), BF),
            pltpu.VMEM((DOM, 1, CAP), jnp.int32),
            pltpu.VMEM((DOM, 1, CAP), jnp.int32),
            pltpu.VMEM((DOM, 8, CAP), BF),
            pltpu.VMEM((DOM, FEAT_DEV, 8, CAP), BF),
            pltpu.VMEM((8, 256), BF),
            pltpu.VMEM((FEAT_DEV, 8, 256), BF),
            pltpu.VMEM((256, 256), BF),
            pltpu.VMEM((256, 256), BF),
            pltpu.VMEM((2, 256), F32),
            pltpu.VMEM((FEAT_DEV, 2, 256), F32),
            pltpu.VMEM((DOM * CAP, 512), BF),
            pltpu.VMEM((FEAT_DEV, 2, 128), F32),
            pltpu.VMEM((FEAT_DEV, 2, 128), F32),
            dma, dma, dma, dma((CHUNKS,)), dma((4,)), dma((4,)),
            dma((2, 4, CHUNKS)), dma((2, 4, CHUNKS)), dma((9, CHUNKS)), dma((9, CHUNKS)),
            dma, dma,
        ],
        compiler_params=pltpu.CompilerParams(
            collective_id=0, has_side_effects=True, vmem_limit_bytes=48 * 1024 * 1024
        ),
    )(
        features, seed_rows.reshape(1, -1), want_rows[0], live_counts, hop_one, hop_two, w1_self, w1_neigh,
        b1.reshape(1, -1), w2_self.T, w2_neigh.T, b2.reshape(1, -1),
    )


def solution(mesh):
    return jax.shard_map(
        per_device,
        mesh=mesh,
        in_specs=(
            P("feat", "dom"),
            P("dom"),
            P("dom", None, None),
            P("dom", None),
            P(None, "dom"),
            P(None, None, "dom"),
            P(),
            P(),
            P("feat"),
            P(None, "feat"),
            P(None, "feat"),
            P("feat"),
        ),
        out_specs=P("feat", "dom"),
        check_vma=False,
    )
```

```python
import jax
import jax.numpy as jnp
from jax import lax
from jax.experimental import pallas as pl
from jax.experimental.pallas import tpu as pltpu
from jax.sharding import PartitionSpec as P

OUT = 256
FAN1 = 15
FAN2 = 10
CAP = 128
DOM = 32
FEAT_DEV = 16
RING = 8
CHUNKS = 4
PER = DOM // CHUNKS
ORDER = (0, 3, 1, 2)
MESH = pl.DeviceIdType.MESH
BF = jnp.bfloat16
F32 = jnp.float32


def iota(shape, dim):
    return lax.broadcasted_iota(jnp.int32, shape, dim)


def dot(a, b):
    return jnp.dot(a, b, preferred_element_type=F32)


def halves(x):
    high = x.astype(BF)
    return high, (x - high.astype(F32)).astype(BF)


def thirds(x):
    high = x.astype(BF)
    rest = x - high.astype(F32)
    mid = rest.astype(BF)
    return high, mid, (rest - mid.astype(F32)).astype(BF)


def swap_groups(x):
    row, group = iota((8, 128), 0), iota((8, 128), 1) // 16
    for bit in (1, 2, 4):
        down = pltpu.roll(pltpu.roll(x, bit, 0), 128 - 16 * bit, 1)
        up = pltpu.roll(pltpu.roll(x, 8 - bit, 0), 16 * bit, 1)
        low_row, low_group = (row & bit) == 0, (group & bit) == 0
        x = jnp.where(low_row == low_group, x, jnp.where(low_row, up, down))
    return x


def kernel(
    tab_in, seed_in, want_in, live_in, hop1_in, hop2_in, w1s_in, w1n_in, b1_in, w2s_in, w2n_in, b2_in,
    out_ref,
    tab_ref, seed_ref, want_ref, live_ref, hop1_ref, hop2_ref, w1s_ref, w1n_ref, b1_ref, b2_ref,
    table, wants, asked, picked, fetched, seeds_own, seeds_all, w2s_all, w2n_all, bias_own, bias_all, counts,
    outgoing, incoming,
    load_sem, ask_send, ask_recv, pick_send, pick_recv, small_send, small_recv, ring_send, ring_recv, pair_send,
    pair_recv, last_send, last_recv,
):
    me_dom, me = lax.axis_index("dom"), lax.axis_index("feat")
    z, core = me // 2, lax.rem(me, 2)

    def remote(src, dst, send, recv, **where):
        return pltpu.make_async_remote_copy(
            src_ref=src, dst_ref=dst, send_sem=send, recv_sem=recv, device_id=where, device_id_type=MESH
        )

    barrier = pltpu.get_barrier_semaphore()

    def greet(i, _):
        pl.semaphore_signal(barrier, inc=1, device_id={"dom": lax.rem(me_dom + i, DOM)}, device_id_type=MESH)
        return 0

    def greet_feat(i, _):
        pl.semaphore_signal(barrier, inc=1, device_id={"feat": lax.rem(me + i, FEAT_DEV)}, device_id_type=MESH)
        return 0

    loads = [
        pltpu.make_async_copy(src, dst, load_sem.at[k])
        for k, (src, dst) in enumerate(
            (
                (want_in, want_ref), (live_in, live_ref), (tab_in, tab_ref), (seed_in, seed_ref), (b1_in, b1_ref),
                (b2_in, b2_ref), (hop1_in, hop1_ref), (hop2_in, hop2_ref), (w1s_in, w1s_ref), (w1n_in, w1n_ref),
            )
        )
    ]
    for load in loads:
        load.start()
    lax.fori_loop(1, DOM, greet, 0)
    lax.fori_loop(1, FEAT_DEV, greet_feat, 0)

    loads[0].wait()
    loads[1].wait()
    eye = iota((DOM, DOM), 0) == iota((DOM, DOM), 1)
    live = jnp.where(eye, jnp.broadcast_to(live_ref[...].astype(F32), (DOM, DOM)), 0.0)
    live = jnp.sum(live, axis=1, keepdims=True).astype(jnp.int32)
    asks = jnp.where(iota((DOM, CAP), 1) < live, want_ref[...], -1)
    wants[...] = asks.reshape(DOM, 1, CAP)

    loads[4].wait()
    loads[5].wait()
    spot = (iota((16, OUT), 1) == iota((16, OUT), 0) + 16 * me).astype(BF)
    for row, ref in enumerate((b1_ref, b2_ref)):
        placed = sum(dot(part, spot) for part in thirds(jnp.broadcast_to(ref[...], (8, 16))))
        bias_own[row : row + 1, :] = placed[0:1]

    pl.semaphore_wait(barrier, DOM - 1 + FEAT_DEV - 1)

    own_ask = pltpu.make_async_copy(wants.at[me_dom], asked.at[0], ask_recv.at[0])
    own_ask.start()
    for group in ORDER:

        def ask(i, _, group=group):
            to = lax.rem(me_dom + i, DOM)
            remote(wants.at[to], asked.at[i], ask_send, ask_recv.at[group], dom=to).start()
            return 0

        lax.fori_loop(max(1, PER * group), PER * (group + 1), ask, 0)

    loads[2].wait()
    for pair in range(32):
        left = tab_ref[:, pl.ds(512 * pair, 256)]
        right = tab_ref[:, pl.ds(512 * pair + 256, 256)]
        table[pl.ds(16 * pair, 16), :] = jnp.concatenate([left, right], axis=0)

    def pick(rows):
        low = jnp.where(rows >= 0, rows & 255, -1)
        high = jnp.broadcast_to(rows >> 8, (8, 256))
        chosen = (iota((256, 256), 0) == low).astype(BF)
        found = dot(table[...], chosen)
        parts = [found[8 * h : 8 * h + 8] for h in range(64)]
        for bit in range(6):
            upper = (high & (1 << bit)) != 0
            parts = [jnp.where(upper, parts[2 * i + 1], parts[2 * i]) for i in range(len(parts) // 2)]
        return parts[0].astype(BF)

    loads[3].wait()
    seeds_own[...] = pick(seed_ref[...])

    w2_rows = pl.ds(pl.multiple_of(16 * me, 16), 16)
    small = (
        (seeds_own, seeds_all.at[me]),
        (w2s_in, w2s_all.at[w2_rows, :]),
        (w2n_in, w2n_all.at[w2_rows, :]),
        (bias_own, bias_all.at[me]),
    )
    for kind, (src, dst) in enumerate(small):
        pltpu.make_async_copy(src, dst, small_recv.at[kind]).start()

    def spread(i, _):
        to = lax.rem(me + i, FEAT_DEV)
        for kind, (src, dst) in enumerate(small):
            remote(src, dst, small_send.at[kind], small_recv.at[kind], feat=to).start()
        return 0

    lax.fori_loop(1, FEAT_DEV, spread, 0)

    for k in range(6, 10):
        loads[k].wait()
    mine = (iota((256, 256), 0) == lax.rem(iota((256, 256), 1), 16) + 16 * me).astype(BF)
    keep = iota((FAN1, 256), 1) // 16 == iota((FAN1, 256), 0)

    def row_of(hops):
        high = dot((hops >> 7).astype(F32).astype(BF), mine)
        low = dot((hops & 127).astype(F32).astype(BF), mine)
        place = jnp.sum(jnp.where(keep, high * 128.0 + low, 0.0), axis=0, keepdims=True).astype(jnp.int32)
        place = (place - me_dom * CAP) & (DOM * CAP - 1)
        place = jnp.where(iota((1, 256), 1) < 16 * FAN1, place, -1)
        return jnp.broadcast_to(place, (16, 256)).astype(jnp.int16)

    first = row_of(hop1_ref[...])
    second = [row_of(hop2_ref[k]) for k in range(FAN2)]

    one, zero = jnp.ones((16, 256), BF), jnp.zeros((16, 256), BF)

    def count(block, _):
        place = (iota((16, 256), 0) + block * 16).astype(jnp.int16)
        total = jnp.where(second[0] == place, one, zero)
        for row in second[1:]:
            total = total + jnp.where(row == place, one, zero)
        rows = pl.ds(pl.multiple_of(block * 16, 16), 16)
        counts[rows, 0:256] = jnp.where(first == place, one, zero)
        counts[rows, 256:512] = total
        return 0

    lax.fori_loop(0, DOM * CAP // 16, count, 0)

    def serve_pair(i, local):
        slot = 2 * i
        got = pick(jnp.concatenate([asked[slot], asked[slot + 1]], axis=1))
        for half in range(2):
            picked[slot + half] = got[:, 128 * half : 128 * half + 128]
            recv = pick_recv.at[slot // PER]
            if local and half == 0:
                pltpu.make_async_copy(picked.at[slot], fetched.at[slot, me], recv).start()
            else:
                to = lax.rem(me_dom + DOM - slot - half, DOM)
                remote(picked.at[slot + half], fetched.at[slot + half, me], pick_send, recv, dom=to).start()
        return 0

    def owners(q):
        return pl.ds(PER * q, PER)

    for group in ORDER:
        pltpu.make_async_copy(asked.at[owners(group)], asked.at[owners(group)], ask_recv.at[group]).wait()
        start = PER // 2 * group
        if group == 0:
            serve_pair(0, True)
            start += 1
        lax.fori_loop(start, PER // 2 * (group + 1), lambda i, _: serve_pair(i, False), 0)

    def block(q, away):
        return fetched.at[owners(q), lax.rem(z + RING + away, RING) * 2 + core]

    partner = 2 * z + 1 - core
    started = []

    def go(copy):
        copy.start()
        started.append(copy)

    CAME = {0: (-1, -1), 1: (1, 1), 2: (-2, -2), 3: (2, 2), 4: (-3, -1), 5: (3, 1)}

    def flow(kind, q):
        if kind == 6:
            away, by = (4, -2) if q % 2 == 0 else (4, 2)
        else:
            away, by = CAME[kind]
        at = block(q, away - by)
        to = lax.rem(z + RING - by, RING) * 2 + core
        return remote(at, at, ring_send.at[kind, q], ring_recv.at[kind, q], feat=to)

    def arrival(kind, q):
        away = 4 if kind == 6 else CAME[kind][0]
        at = block(q, away)
        return remote(at, at, ring_send.at[kind, q], ring_recv.at[kind, q], feat=partner)

    def to_partner(kind, q):
        away = 0 if kind == 7 else 4 if kind == 6 else CAME[kind][0]
        at = block(q, away)
        return remote(at, at, pair_send.at[kind, q], pair_recv.at[kind, q], feat=partner)

    def begin(q):
        pltpu.make_async_copy(block(q, 0), block(q, 1), pick_recv.at[q]).wait()
        for kind in (2, 3, 0, 1):
            go(flow(kind, q))
        go(to_partner(7, q))

    def relay(q):
        for kind in (2, 3):
            arrival(kind, q).wait_recv()
            go(flow(kind + 2, q))
            if q % 2 == kind % 2:
                go(flow(6, q))
            go(to_partner(kind, q))

    def finish(q):
        for kind in (0, 1, 4, 5, 6):
            arrival(kind, q).wait_recv()
            go(to_partner(kind, q))

    a, b, c, d = ORDER
    begin(a)
    begin(b)
    relay(a)
    relay(b)
    begin(c)
    begin(d)
    finish(a)
    finish(b)
    relay(c)
    relay(d)
    finish(c)
    finish(d)

    total = jnp.zeros((128, 512), F32)
    for q in ORDER:
        for kind in range(8):
            to_partner(kind, q).wait_recv()
        for pair in range(PER // 2):
            o = PER * q + 2 * pair
            left = fetched[o].reshape(128, CAP)
            right = fetched[o + 1].reshape(128, CAP)
            total = total + dot(jnp.concatenate([left, right], axis=1), counts[pl.ds(o * CAP, 256), :])

    for kind, whole in enumerate((seeds_all, w2s_all, w2n_all, bias_all)):
        pltpu.make_async_copy(whole, whole, small_recv.at[kind]).wait()

    seed_lane = iota((256, 256), 1) - 16 * FAN1
    own_seeds = ((iota((256, 256), 0) == seed_lane + 16 * me) & (seed_lane >= 0)).astype(BF)
    selves = (total[:, :256] + dot(seeds_all[...].reshape(128, 256), own_seeds)).T
    sums = total[:, 256:].T
    one_sum = selves[0:16]
    for j in range(1, FAN1):
        one_sum = one_sum + selves[16 * j : 16 * j + 16]
    means = jnp.concatenate([sums[: 16 * FAN1] * (1.0 / FAN2), one_sum * (1.0 / FAN1)], axis=0).astype(BF)
    selves = selves.astype(BF)

    def nt(a, b):
        return lax.dot_general(a, b, (((1,), (1,)), ((), ())), preferred_element_type=F32)

    biases = jnp.sum(bias_all[...], axis=0)
    hidden = nt(selves, w1s_ref[...]) + nt(means, w1n_ref[...])
    hidden = jnp.maximum(hidden + biases[0:1], 0.0)
    g = hidden[0:16]
    for j in range(1, FAN1):
        g = g + hidden[16 * j : 16 * j + 16]
    g = g * (1.0 / FAN1)
    h_seed = hidden[16 * FAN1 :]
    z_out = biases[1:2]
    for part in halves(h_seed):
        z_out = z_out + dot(part, w2s_all[...])
    for part in halves(g):
        z_out = z_out + dot(part, w2n_all[...])
    square = jnp.sum(z_out * z_out, axis=1, keepdims=True)
    embed = z_out * lax.rsqrt(square * (1.0 / OUT) + 1.0)

    for a in range(2):
        for h in range(2):
            turned = swap_groups(embed[8 * a : 8 * a + 8, 128 * h : 128 * h + 128])
            outgoing[8 * h : 8 * h + 8, a, :] = turned

    pltpu.make_async_copy(outgoing.at[me], incoming.at[me], last_recv).start()

    def hand(i, _):
        to = lax.rem(me + i, FEAT_DEV)
        remote(outgoing.at[to], incoming.at[me], last_send, last_recv, feat=to).start()
        return 0

    lax.fori_loop(1, FEAT_DEV, hand, 0)
    pltpu.make_async_copy(outgoing, incoming, last_recv).wait()

    came = incoming[...].reshape(32, 128).T
    widen = (iota((32, 256), 1) // 8 == iota((32, 256), 0)).astype(BF)
    wide = sum(dot(part, widen) for part in thirds(came))
    lane = lax.rem(iota((16, 256), 1), 8)
    result = jnp.zeros((16, 256), F32)
    for b in range(8):
        result = result + jnp.where(lane == b, wide[16 * b : 16 * b + 16], 0.0)
    out_ref[...] = result

    for copy in started:
        copy.wait_send()
    others = pl.ds(0, DOM - 1)
    pltpu.make_async_copy(wants.at[others], wants.at[others], ask_send).wait()
    pltpu.make_async_copy(picked.at[others], picked.at[others], pick_send).wait()
    peers = pl.ds(0, FEAT_DEV - 1)
    rows = pl.ds(0, 16 * (FEAT_DEV - 1))
    pltpu.make_async_copy(seeds_all.at[peers], seeds_all.at[peers], small_send.at[0]).wait()
    pltpu.make_async_copy(w2s_all.at[rows, :], w2s_all.at[rows, :], small_send.at[1]).wait()
    pltpu.make_async_copy(w2n_all.at[rows, :], w2n_all.at[rows, :], small_send.at[2]).wait()
    pltpu.make_async_copy(bias_all.at[peers], bias_all.at[peers], small_send.at[3]).wait()
    pltpu.make_async_copy(outgoing.at[peers], outgoing.at[peers], last_send).wait()


def per_device(
    features, seed_rows, want_rows, live_counts, hop_one, hop_two, w1_self, w1_neigh, b1, w2_self, w2_neigh, b2
):
    hbm = pl.BlockSpec(memory_space=pltpu.HBM)
    dma = pltpu.SemaphoreType.DMA
    args = (
        features, seed_rows.reshape(1, -1), want_rows[0], live_counts, hop_one, hop_two, w1_self, w1_neigh,
        b1.reshape(1, -1), w2_self.T, w2_neigh.T, b2.reshape(1, -1),
    )
    return pl.pallas_call(
        kernel,
        out_shape=jax.ShapeDtypeStruct((16, 256), F32),
        in_specs=[hbm] * 12,
        out_specs=pl.BlockSpec(memory_space=pltpu.VMEM),
        scratch_shapes=[
            *(pltpu.VMEM(args[k].shape, args[k].dtype) for k in (0, 1, 2, 3, 4, 5, 6, 7, 8, 11)),
            pltpu.VMEM((512, 256), BF),
            pltpu.VMEM((DOM, 1, CAP), jnp.int32),
            pltpu.VMEM((DOM, 1, CAP), jnp.int32),
            pltpu.VMEM((DOM, 8, CAP), BF),
            pltpu.VMEM((DOM, FEAT_DEV, 8, CAP), BF),
            pltpu.VMEM((8, 256), BF),
            pltpu.VMEM((FEAT_DEV, 8, 256), BF),
            pltpu.VMEM((256, 256), BF),
            pltpu.VMEM((256, 256), BF),
            pltpu.VMEM((2, 256), F32),
            pltpu.VMEM((FEAT_DEV, 2, 256), F32),
            pltpu.VMEM((DOM * CAP, 512), BF),
            pltpu.VMEM((FEAT_DEV, 2, 128), F32),
            pltpu.VMEM((FEAT_DEV, 2, 128), F32),
            dma((10,)), dma, dma((CHUNKS,)), dma, dma((CHUNKS,)), dma((4,)), dma((4,)),
            dma((7, CHUNKS)), dma((7, CHUNKS)), dma((8, CHUNKS)), dma((8, CHUNKS)), dma, dma,
        ],
        compiler_params=pltpu.CompilerParams(
            collective_id=0, has_side_effects=True, vmem_limit_bytes=60 * 1024 * 1024
        ),
    )(*args)


def solution(mesh):
    return jax.shard_map(
        per_device,
        mesh=mesh,
        in_specs=(
            P("feat", "dom"),
            P("dom"),
            P("dom", None, None),
            P("dom", None),
            P(None, "dom"),
            P(None, None, "dom"),
            P(),
            P(),
            P("feat"),
            P(None, "feat"),
            P(None, "feat"),
            P("feat"),
        ),
        out_specs=P("feat", "dom"),
        check_vma=False,
    )
```

```python
import jax
import jax.numpy as jnp
from jax import lax
from jax.experimental import pallas as pl
from jax.experimental.pallas import tpu as pltpu
from jax.sharding import PartitionSpec as P

OUT = 256
FAN1 = 15
FAN2 = 10
CAP = 128
DOM = 32
FEAT_DEV = 16
RING = 8
CHUNKS = 8
PER = DOM // CHUNKS
ORDER = (0, 7, 1, 6, 2, 5, 3, 4)
RELAY, DIRECT = 0, 1
MODE = dict(zip(ORDER, (0, 0, 0, 0, 0, 1, 1, 1)))
AWAY = (-1, 1, -2, 2, -3, 3, 4)
LAG = 4
MESH = pl.DeviceIdType.MESH
BF = jnp.bfloat16
F32 = jnp.float32


def iota(shape, dim):
    return lax.broadcasted_iota(jnp.int32, shape, dim)


def dot(a, b):
    return jnp.dot(a, b, preferred_element_type=F32)


def halves(x):
    high = x.astype(BF)
    return high, (x - high.astype(F32)).astype(BF)


def thirds(x):
    high = x.astype(BF)
    rest = x - high.astype(F32)
    mid = rest.astype(BF)
    return high, mid, (rest - mid.astype(F32)).astype(BF)


def swap_groups(x):
    row, group = iota((8, 128), 0), iota((8, 128), 1) // 16
    for bit in (1, 2, 4):
        down = pltpu.roll(pltpu.roll(x, bit, 0), 128 - 16 * bit, 1)
        up = pltpu.roll(pltpu.roll(x, 8 - bit, 0), 16 * bit, 1)
        low_row, low_group = (row & bit) == 0, (group & bit) == 0
        x = jnp.where(low_row == low_group, x, jnp.where(low_row, up, down))
    return x


def kernel(
    tab_in, seed_in, want_in, live_in, hop1_in, hop2_in, w1s_in, w1n_in, b1_in, w2s_in, w2n_in, b2_in,
    out_ref,
    tab_ref, seed_ref, want_ref, live_ref, hop1_ref, hop2_ref, w1s_ref, w1n_ref, b1_ref, b2_ref,
    table, wants, asked, picked, fetched, seeds_own, seeds_all, w2s_all, w2n_all, bias_own, bias_all, counts,
    outgoing, incoming,
    load_sem, ask_send, ask_recv, pick_send, pick_recv, small_send, small_recv, ring_send, ring_recv, pair_send,
    pair_recv, last_send, last_recv,
):
    me_dom, me = lax.axis_index("dom"), lax.axis_index("feat")
    z, core = me // 2, lax.rem(me, 2)

    def remote(src, dst, send, recv, **where):
        return pltpu.make_async_remote_copy(
            src_ref=src, dst_ref=dst, send_sem=send, recv_sem=recv, device_id=where, device_id_type=MESH
        )

    barrier = pltpu.get_barrier_semaphore()

    def greet(**where):
        pl.semaphore_signal(barrier, inc=1, device_id=where, device_id_type=MESH)

    loads = [
        pltpu.make_async_copy(src, dst, load_sem.at[k])
        for k, (src, dst) in enumerate(
            (
                (want_in, want_ref), (live_in, live_ref), (tab_in, tab_ref), (seed_in, seed_ref), (b1_in, b1_ref),
                (b2_in, b2_ref), (hop1_in, hop1_ref), (hop2_in, hop2_ref), (w1s_in, w1s_ref), (w1n_in, w1n_ref),
            )
        )
    ]
    for load in loads:
        load.start()
    for i in sorted(range(1, DOM), key=lambda i: -min(i, DOM - i)):
        greet(dom=lax.rem(me_dom + i, DOM))
    for i in sorted(range(1, FEAT_DEV), key=lambda i: -min(i, FEAT_DEV - i)):
        greet(feat=lax.rem(me + i, FEAT_DEV))

    loads[0].wait()
    loads[1].wait()
    eye = iota((DOM, DOM), 0) == iota((DOM, DOM), 1)
    live = jnp.where(eye, jnp.broadcast_to(live_ref[...].astype(F32), (DOM, DOM)), 0.0)
    live = jnp.sum(live, axis=1, keepdims=True).astype(jnp.int32)
    asks = jnp.where(iota((DOM, CAP), 1) < live, want_ref[...], -1)
    wants[...] = asks.reshape(DOM, 1, CAP)

    loads[4].wait()
    loads[5].wait()
    spot = (iota((16, OUT), 1) == iota((16, OUT), 0) + 16 * me).astype(BF)
    for row, ref in enumerate((b1_ref, b2_ref)):
        placed = sum(dot(part, spot) for part in thirds(jnp.broadcast_to(ref[...], (8, 16))))
        bias_own[row : row + 1, :] = placed[0:1]

    pl.semaphore_wait(barrier, DOM - 1 + FEAT_DEV - 1)

    own_ask = pltpu.make_async_copy(wants.at[me_dom], asked.at[0], ask_recv.at[0])
    own_ask.start()
    for group in ORDER:

        def ask(i, _, group=group):
            to = lax.rem(me_dom + i, DOM)
            remote(wants.at[to], asked.at[i], ask_send, ask_recv.at[group], dom=to).start()
            return 0

        lax.fori_loop(max(1, PER * group), PER * (group + 1), ask, 0)

    loads[2].wait()
    for pair in range(32):
        left = tab_ref[:, pl.ds(512 * pair, 256)]
        right = tab_ref[:, pl.ds(512 * pair + 256, 256)]
        table[pl.ds(16 * pair, 16), :] = jnp.concatenate([left, right], axis=0)

    def pick(rows):
        low = jnp.where(rows >= 0, rows & 255, -1)
        wide = rows.shape[1]
        high = jnp.broadcast_to(rows >> 8, (8, wide))
        chosen = (iota((256, wide), 0) == low).astype(BF)
        found = dot(table[...], chosen)
        parts = [found[8 * h : 8 * h + 8] for h in range(64)]
        for bit in range(6):
            upper = (high & (1 << bit)) != 0
            parts = [jnp.where(upper, parts[2 * i + 1], parts[2 * i]) for i in range(len(parts) // 2)]
        return parts[0].astype(BF)

    loads[3].wait()
    seeds_own[...] = pick(seed_ref[...])

    w2_rows = pl.ds(pl.multiple_of(16 * me, 16), 16)
    small = (
        (seeds_own, seeds_all.at[me]),
        (w2s_in, w2s_all.at[w2_rows, :]),
        (w2n_in, w2n_all.at[w2_rows, :]),
        (bias_own, bias_all.at[me]),
    )
    for kind, (src, dst) in enumerate(small):
        pltpu.make_async_copy(src, dst, small_recv.at[kind]).start()

    def spread(i, _):
        to = lax.rem(me + i, FEAT_DEV)
        for kind, (src, dst) in enumerate(small):
            remote(src, dst, small_send.at[kind], small_recv.at[kind], feat=to).start()
        return 0

    lax.fori_loop(1, FEAT_DEV, spread, 0)

    for k in range(6, 10):
        loads[k].wait()
    mine = (iota((256, 256), 0) == lax.rem(iota((256, 256), 1), 16) + 16 * me).astype(BF)
    keep = iota((FAN1, 256), 1) // 16 == iota((FAN1, 256), 0)

    def row_of(hops):
        high = dot((hops >> 7).astype(F32).astype(BF), mine)
        low = dot((hops & 127).astype(F32).astype(BF), mine)
        place = jnp.sum(jnp.where(keep, high * 128.0 + low, 0.0), axis=0, keepdims=True).astype(jnp.int32)
        place = (place - me_dom * CAP) & (DOM * CAP - 1)
        place = jnp.where(iota((1, 256), 1) < 16 * FAN1, place, -1)
        return jnp.broadcast_to(place, (16, 256)).astype(jnp.int16)

    first = row_of(hop1_ref[...])
    second = [row_of(hop2_ref[k]) for k in range(FAN2)]

    one, zero = jnp.ones((16, 256), BF), jnp.zeros((16, 256), BF)

    def count(owner, _):
        for part in range(CAP // 16):
            base = owner * CAP + part * 16
            place = (iota((16, 256), 0) + base).astype(jnp.int16)
            total = jnp.where(second[0] == place, one, zero)
            for row in second[1:]:
                total = total + jnp.where(row == place, one, zero)
            rows = pl.ds(pl.multiple_of(base, 16), 16)
            counts[rows, 0:256] = jnp.where(first == place, one, zero)
            counts[rows, 256:512] = total
        return 0

    counted = [0]

    def count_some(n):
        lax.fori_loop(counted[0], counted[0] + n, count, 0)
        counted[0] += n

    def owners(q):
        return pl.ds(PER * q, PER)

    def serve(group):
        pltpu.make_async_copy(asked.at[owners(group)], asked.at[owners(group)], ask_recv.at[group]).wait()
        slots = range(PER * group, PER * (group + 1))
        got = pick(jnp.concatenate([asked[slot] for slot in slots], axis=1))
        for k, slot in enumerate(slots):
            picked[slot] = got[:, CAP * k : CAP * (k + 1)]
        for slot in slots:
            to = lax.rem(me_dom + DOM - slot, DOM)
            if slot == 0:
                pltpu.make_async_copy(picked.at[slot], fetched.at[slot, me], pick_recv.at[group]).start()
            else:
                remote(picked.at[slot], fetched.at[slot, me], pick_send, pick_recv.at[group], dom=to).start()

    count_some(DOM)
    for group in ORDER[:4]:
        serve(group)
    for group in ORDER[4:]:
        serve(group)

    def block(q, away):
        return fetched.at[owners(q), lax.rem(z + RING + away, RING) * 2 + core]

    partner = 2 * z + 1 - core
    started = []

    def go(copy):
        copy.start()
        started.append(copy)

    def source(kind, q):
        if MODE[q] != RELAY or kind < 4:
            return AWAY[kind]
        return {4: -1, 5: 1, 6: -2 if ORDER.index(q) % 2 == 0 else 2}[kind]

    def flow(kind, q):
        by = source(kind, q)
        at = block(q, AWAY[kind] - by)
        to = lax.rem(z + RING - by, RING) * 2 + core
        return remote(at, at, ring_send.at[kind, q], ring_recv.at[kind, q], feat=to)

    def arrival(kind, q):
        at = block(q, AWAY[kind])
        return remote(at, at, ring_send.at[kind, q], ring_recv.at[kind, q], feat=partner)

    def to_partner(kind, q):
        at = block(q, 0 if kind == 7 else AWAY[kind])
        return remote(at, at, pair_send.at[kind, q], pair_recv.at[kind, q], feat=partner)

    def begin(q):
        pltpu.make_async_copy(block(q, 0), block(q, 1), pick_recv.at[q]).wait()
        for kind in {RELAY: (2, 3, 0, 1), DIRECT: (6, 4, 5, 2, 3, 0, 1)}[MODE[q]]:
            go(flow(kind, q))
        go(to_partner(7, q))

    def relay(q):
        for kind in (2, 3):
            arrival(kind, q).wait_recv()
            go(flow(kind + 2, q))
            if source(6, q) == AWAY[kind]:
                go(flow(6, q))
            go(to_partner(kind, q))

    def finish(q):
        for kind in (0, 1, 4, 5, 6) if MODE[q] == RELAY else (0, 1, 2, 3, 4, 5, 6):
            arrival(kind, q).wait_recv()
            go(to_partner(kind, q))

    relays = [q for q in ORDER if MODE[q] == RELAY]
    for step in range(8 + LAG):
        if step < 8:
            begin(ORDER[step])
        if LAG <= step < LAG + len(relays):
            relay(relays[step - LAG])
    for step, q in enumerate(ORDER):
        finish(q)

    total = jnp.zeros((128, 512), F32)
    for q in ORDER:
        for kind in range(8):
            to_partner(kind, q).wait_recv()
        for pair in range(PER // 2):
            o = PER * q + 2 * pair
            left = fetched[o].reshape(128, CAP)
            right = fetched[o + 1].reshape(128, CAP)
            total = total + dot(jnp.concatenate([left, right], axis=1), counts[pl.ds(o * CAP, 256), :])

    for kind, whole in enumerate((seeds_all, w2s_all, w2n_all, bias_all)):
        pltpu.make_async_copy(whole, whole, small_recv.at[kind]).wait()

    seed_lane = iota((256, 256), 1) - 16 * FAN1
    own_seeds = ((iota((256, 256), 0) == seed_lane + 16 * me) & (seed_lane >= 0)).astype(BF)
    selves = (total[:, :256] + dot(seeds_all[...].reshape(128, 256), own_seeds)).T
    sums = total[:, 256:].T
    one_sum = selves[0:16]
    for j in range(1, FAN1):
        one_sum = one_sum + selves[16 * j : 16 * j + 16]
    means = jnp.concatenate([sums[: 16 * FAN1] * (1.0 / FAN2), one_sum * (1.0 / FAN1)], axis=0).astype(BF)
    selves = selves.astype(BF)

    def nt(a, b):
        return lax.dot_general(a, b, (((1,), (1,)), ((), ())), preferred_element_type=F32)

    biases = jnp.sum(bias_all[...], axis=0)
    hidden = nt(selves, w1s_ref[...]) + nt(means, w1n_ref[...])
    hidden = jnp.maximum(hidden + biases[0:1], 0.0)
    g = hidden[0:16]
    for j in range(1, FAN1):
        g = g + hidden[16 * j : 16 * j + 16]
    g = g * (1.0 / FAN1)
    h_seed = hidden[16 * FAN1 :]
    z_out = biases[1:2]
    for part in halves(h_seed):
        z_out = z_out + dot(part, w2s_all[...])
    for part in halves(g):
        z_out = z_out + dot(part, w2n_all[...])
    square = jnp.sum(z_out * z_out, axis=1, keepdims=True)
    embed = z_out * lax.rsqrt(square * (1.0 / OUT) + 1.0)

    for a in range(2):
        for h in range(2):
            turned = swap_groups(embed[8 * a : 8 * a + 8, 128 * h : 128 * h + 128])
            outgoing[8 * h : 8 * h + 8, a, :] = turned

    pltpu.make_async_copy(outgoing.at[me], incoming.at[me], last_recv).start()

    def hand(i, _):
        to = lax.rem(me + i, FEAT_DEV)
        remote(outgoing.at[to], incoming.at[me], last_send, last_recv, feat=to).start()
        return 0

    lax.fori_loop(1, FEAT_DEV, hand, 0)
    for copy in started:
        copy.wait_send()
    others = pl.ds(0, DOM - 1)
    pltpu.make_async_copy(wants.at[others], wants.at[others], ask_send).wait()
    pltpu.make_async_copy(picked.at[others], picked.at[others], pick_send).wait()
    peers = pl.ds(0, FEAT_DEV - 1)
    rows = pl.ds(0, 16 * (FEAT_DEV - 1))
    pltpu.make_async_copy(seeds_all.at[peers], seeds_all.at[peers], small_send.at[0]).wait()
    pltpu.make_async_copy(w2s_all.at[rows, :], w2s_all.at[rows, :], small_send.at[1]).wait()
    pltpu.make_async_copy(w2n_all.at[rows, :], w2n_all.at[rows, :], small_send.at[2]).wait()
    pltpu.make_async_copy(bias_all.at[peers], bias_all.at[peers], small_send.at[3]).wait()

    pltpu.make_async_copy(outgoing, incoming, last_recv).wait()

    came = incoming[...].reshape(32, 128).T
    widen = (iota((32, 256), 1) // 8 == iota((32, 256), 0)).astype(BF)
    wide = sum(dot(part, widen) for part in thirds(came))
    lane = lax.rem(iota((16, 256), 1), 8)
    result = jnp.zeros((16, 256), F32)
    for b in range(8):
        result = result + jnp.where(lane == b, wide[16 * b : 16 * b + 16], 0.0)
    out_ref[...] = result
    pltpu.make_async_copy(outgoing.at[peers], outgoing.at[peers], last_send).wait()


def per_device(
    features, seed_rows, want_rows, live_counts, hop_one, hop_two, w1_self, w1_neigh, b1, w2_self, w2_neigh, b2
):
    hbm = pl.BlockSpec(memory_space=pltpu.HBM)
    dma = pltpu.SemaphoreType.DMA
    args = (
        features, seed_rows.reshape(1, -1), want_rows[0], live_counts, hop_one, hop_two, w1_self, w1_neigh,
        b1.reshape(1, -1), w2_self.T, w2_neigh.T, b2.reshape(1, -1),
    )
    return pl.pallas_call(
        kernel,
        out_shape=jax.ShapeDtypeStruct((16, 256), F32),
        in_specs=[hbm] * 12,
        out_specs=pl.BlockSpec(memory_space=pltpu.VMEM),
        scratch_shapes=[
            *(pltpu.VMEM(args[k].shape, args[k].dtype) for k in (0, 1, 2, 3, 4, 5, 6, 7, 8, 11)),
            pltpu.VMEM((512, 256), BF),
            pltpu.VMEM((DOM, 1, CAP), jnp.int32),
            pltpu.VMEM((DOM, 1, CAP), jnp.int32),
            pltpu.VMEM((DOM, 8, CAP), BF),
            pltpu.VMEM((DOM, FEAT_DEV, 8, CAP), BF),
            pltpu.VMEM((8, 256), BF),
            pltpu.VMEM((FEAT_DEV, 8, 256), BF),
            pltpu.VMEM((256, 256), BF),
            pltpu.VMEM((256, 256), BF),
            pltpu.VMEM((2, 256), F32),
            pltpu.VMEM((FEAT_DEV, 2, 256), F32),
            pltpu.VMEM((DOM * CAP, 512), BF),
            pltpu.VMEM((FEAT_DEV, 2, 128), F32),
            pltpu.VMEM((FEAT_DEV, 2, 128), F32),
            dma((10,)), dma, dma((CHUNKS,)), dma, dma((CHUNKS,)), dma((4,)), dma((4,)),
            dma((7, CHUNKS)), dma((7, CHUNKS)), dma((8, CHUNKS)), dma((8, CHUNKS)), dma, dma,
        ],
        compiler_params=pltpu.CompilerParams(
            collective_id=0, has_side_effects=True, vmem_limit_bytes=60 * 1024 * 1024
        ),
    )(*args)


def solution(mesh):
    return jax.shard_map(
        per_device,
        mesh=mesh,
        in_specs=(
            P("feat", "dom"),
            P("dom"),
            P("dom", None, None),
            P("dom", None),
            P(None, "dom"),
            P(None, None, "dom"),
            P(),
            P(),
            P("feat"),
            P(None, "feat"),
            P(None, "feat"),
            P("feat"),
        ),
        out_specs=P("feat", "dom"),
        check_vma=False,
    )
```
